32 devices in a mesh: dp: 4 (over z), expert: 8 (over y, x, core).
Axes of the slice: x: 2, y: 2, z: 4, core: 2. Of those that a mesh axis runs over, the one named last changes fastest.
Arguments:
- frames: bfloat16 [4096, 1024], P(('dp', 'expert')), may hold values from -6 to 6
- norm_gain: float32 [1024], replicated, may hold values from 0.5 to 1.5
- norm_bias: float32 [1024], replicated, may hold values from -3 to 3
- routes: int32 [4096, 2], P(('dp', 'expert')), may hold values from 0 to 15, all different within a row; in each aligned block of 128 rows (0 to 127, 128 to 255, ...) at most 32 rows name the same one
- gate_codes: int32 [4096, 2], P(('dp', 'expert')), may hold values from 1 to 255
- limits: int32 [16], replicated, may hold values from 16 to 32
- up_weight: bfloat16 [32, 1024, 2048], P(('dp', 'expert')), may hold values from -0.1875 to 0.1875
- up_bias: float32 [32, 2048], P(('dp', 'expert')), may hold values from -3 to 3
- down_weight: bfloat16 [32, 2048, 1024], P(('dp', 'expert')), may hold values from -0.09375 to 0.09375
- down_bias: float32 [16, 1024], replicated, may hold values from -2 to 2
Outputs:
- mixed: bfloat16 [4096, 1024], P(('dp', 'expert'))
- load: int32 [16], replicated
The draws below stay inside these ranges and needn't reach their ends.
Inputs may be any that keep to these rules, and one draw needn't show every extreme that they name: `routes`: in each aligned block of 128 rows (the rows of one device) no expert is named by more than 32 rows, and some block has an expert named by exactly 32 rows; the two entries of a row differ.
All inputs are finite; a program needn't handle non-finite values.
Results may differ from the reference program's by a relative error of at most 0.0051.
Values may be sent and summed in bfloat16 or wider, within the bound.
A program may use at most 64 MiB of HBM per device.

```python
import math
import jax
import jax.numpy as jnp
import numpy as np
from jax import lax

D = 1024
FF = 4096
TOK_DEV = 128
EXPERTS = 16
SHARDS = 2
FF_DEV = 2048
CAP = 32
TOKENS = 4096
N_DP = 4
N_EXPERT = 8


def plant(array, rng, least, high):
    longest = array.shape.index(max(array.shape))
    spots = []
    for shift in (0, 1):
        where = [jax.random.randint(jax.random.fold_in(rng, axis), (), 0, length) for axis, length in enumerate(array.shape)]
        where[longest] = (where[longest] + shift) % array.shape[longest]
        spots.append(tuple(where))
    return array.at[spots[0]].set(least).at[spots[1]].set(high)


def level_of(own_key, shape, pieces, low, top_value):
    def one(axis_at, shards_of):
        heights = jax.random.uniform(jax.random.fold_in(jax.random.fold_in(own_key, 6), axis_at), (shards_of,), jnp.float32, low / len(pieces), top_value / len(pieces))
        return jnp.repeat(jnp.exp(heights), shape[axis_at] // shards_of).reshape((-1,) + (1,) * (len(shape) - axis_at - 1))

    gain = one(*pieces[0])
    for cut in pieces[1:]:
        gain = gain * one(*cut)
    return gain


def shared_out(key, own, number, rows, number_of, top, limit, skew):
    sequence = jax.random.permutation(key, number_of)
    packed, usual = load_shares(number_of, rows * top, limit, skew, True), load_shares(number_of, rows * top, limit, skew, False)
    places = jnp.arange(number_of)

    def named(lengths, turn):
        used = int((lengths > 0).sum())
        fixed = max(1, used // 4)
        moved = fixed + (places - fixed + turn * (used - fixed)) % max(1, number_of - fixed)
        return jnp.zeros((number_of,), jnp.int32).at[sequence[jnp.where(places < fixed, places, moved)]].set(jnp.asarray(lengths, jnp.int32))

    lengths = jnp.where(number % 4 == 0, named(packed, number // 4), named(usual, number - number // 4 - 1))
    mixed = jax.random.permutation(jax.random.fold_in(own, 3), number_of)
    giver, receiver = mixed[0:number_of // 2 * 2:2], mixed[1:number_of // 2 * 2:2]
    room = jnp.minimum(lengths[giver] - 1, limit - lengths[receiver]) // 2
    room = jnp.where((giver == sequence[0]) | (receiver == sequence[0]) | (lengths[receiver] == 0), 0, jnp.maximum(room, 0))
    moved = jax.random.randint(jax.random.fold_in(own, 4), (number_of // 2,), 0, 1 << 20) % (room + 1)
    lengths = lengths.at[giver].add(-moved).at[receiver].add(moved)
    members = jnp.searchsorted(jnp.cumsum(lengths), jnp.arange(rows * top), side="right").astype(jnp.int32)
    table = members.reshape(top, rows).T
    table = table[jax.random.permutation(jax.random.fold_in(own, 1), rows)]
    turn = jax.random.randint(jax.random.fold_in(own, 2), (rows, 1), 0, top)
    return jnp.take_along_axis(table, (jnp.arange(top)[None, :] + turn) % top, axis=1)


def load_shares(count, total, reach, lean, full):
    portions = [(1 << 20) // math.isqrt(grade ** lean) + 1 for grade in range(1, count + 1)]
    largest = reach if full else min(reach, max(-(-total // count), total * portions[0] // sum(portions)))
    least = 1 if total - largest >= count - 1 else 0
    holding, rest = [largest] + [least] * (count - 1), total - largest - least * (count - 1)
    while rest > 0:
        candidates = [i for i in range(1, count) if holding[i] < largest] or [i for i in range(1, count) if holding[i] < reach]
        whole, left = sum([portions[i] for i in candidates]), rest
        for i in candidates:
            extra = min(reach - holding[i], max(1, left * portions[i] // whole), rest)
            holding[i] = holding[i] + extra
            rest = rest - extra
    return np.array(holding)


def gaussian(stream_key, dims, scale, bound, shards=(), held_as=jnp.bfloat16):
    values = scale * jax.random.normal(stream_key, dims, jnp.float32)
    if shards:
        values = values * level_of(stream_key, dims, shards, -0.22, 0.18)
    return jnp.clip(values, -bound, bound).astype(held_as)


def setup_inputs(seed: int = 0) -> dict:
    keys = jax.random.split(jax.random.key(seed), 11)
    frames = gaussian(keys[0], (TOKENS, D), 1.0, 6.0, ((0, 32),))
    norm_gain = jnp.clip(jax.random.uniform(keys[1], (D,), jnp.float32, 0.5, 1.5), 0.5, 1.5)
    norm_bias = gaussian(keys[2], (D,), 0.5, 3.0, (), jnp.float32)
    routes_keys = jax.random.split(jax.random.fold_in(keys[3], 1), TOKENS // TOK_DEV)
    routes_turns = jax.random.permutation(jax.random.fold_in(keys[3], 3), TOKENS // TOK_DEV)
    routes = jax.vmap(lambda own, number: shared_out(jax.random.fold_in(keys[3], 2), own, number, TOK_DEV, EXPERTS, 2, CAP, 2))(routes_keys, routes_turns).reshape((TOKENS, 2))
    gate_codes = plant(jax.random.randint(keys[4], (TOKENS, 2), 1, 256), jax.random.fold_in(keys[4], 1), 1, 255).astype(jnp.int32)
    limits = plant(jax.random.randint(keys[5], (EXPERTS,), CAP // 2, CAP + 1), jax.random.fold_in(keys[5], 1), CAP // 2, CAP).astype(jnp.int32)
    up_weight = gaussian(keys[6], (EXPERTS * SHARDS, D, FF_DEV), D ** -0.5, 0.1875, ((0, 32),))
    up_bias = gaussian(keys[7], (EXPERTS * SHARDS, FF_DEV), 0.5, 3.0, ((0, 32),), jnp.float32)
    down_weight = gaussian(keys[8], (EXPERTS * SHARDS, FF_DEV, D), FF ** -0.5, 0.09375, ((0, 32),))
    down_bias = gaussian(keys[9], (EXPERTS, D), 0.3, 2.0, (), jnp.float32)
    return dict(frames=frames, norm_gain=norm_gain, norm_bias=norm_bias, routes=routes, gate_codes=gate_codes, limits=limits, up_weight=up_weight, up_bias=up_bias, down_weight=down_weight, down_bias=down_bias)


epsilon = 1e-05

def layer_norm(frames, norm_gain, norm_bias):
    values = frames.astype(jnp.float32)
    center = lax.optimization_barrier(jnp.mean(values, axis=-1, keepdims=True))
    shifted = values - center
    spread = lax.optimization_barrier(jnp.mean(shifted * shifted, axis=-1, keepdims=True))
    return (shifted * lax.rsqrt(spread + epsilon) * norm_gain + norm_bias).astype(jnp.bfloat16)

def place_slots(routes_block, limits, expert_total, capacity):
    flat_routes = routes_block.reshape(-1)
    expert_ids = jnp.arange(expert_total, dtype=jnp.int32)
    expert_hits = (flat_routes[:, None] == expert_ids[None, :]).astype(jnp.int32)
    earlier = jnp.cumsum(expert_hits, axis=0).astype(jnp.int32) - expert_hits
    slot_rank = lax.optimization_barrier(jnp.sum(earlier * expert_hits, axis=1)).astype(jnp.int32)
    slot_bound = lax.optimization_barrier(jnp.sum(expert_hits * limits[None, :], axis=1)).astype(jnp.int32)
    kept_mask = (slot_rank < slot_bound).astype(jnp.int32)
    slot_index = jnp.minimum(flat_routes * capacity + slot_rank, expert_total * capacity - 1).astype(jnp.int32)
    slot_ids = jnp.arange(expert_total * capacity, dtype=jnp.int32)
    matches = (slot_index[None, :] == slot_ids[:, None]).astype(jnp.int32) * kept_mask[None, :]
    frame_ids = jnp.arange(flat_routes.shape[0], dtype=jnp.int32) // 2
    source_frame = lax.optimization_barrier(jnp.sum(matches * frame_ids[None, :], axis=1)).astype(jnp.int32)
    filled = lax.optimization_barrier(jnp.sum(matches, axis=1)).astype(jnp.int32)
    expert_loads = lax.optimization_barrier(jnp.sum(expert_hits * kept_mask[:, None], axis=0)).astype(jnp.int32)
    return (slot_index, kept_mask, source_frame, filled, expert_loads)

def fill_slots(normed_block, source_frame, filled):
    slot_rows = jnp.take(normed_block, source_frame, axis=0)
    return slot_rows * filled[:, None].astype(jnp.bfloat16)

def combine(frames_block, returned, slot_index, kept_mask, gate_block):
    code_values = gate_block.astype(jnp.float32)
    shares = code_values / lax.optimization_barrier(jnp.sum(code_values, axis=1, keepdims=True))
    weights = shares.reshape(-1) * kept_mask.astype(jnp.float32)
    picked = jnp.take(returned, slot_index, axis=0).astype(jnp.float32)
    weighted = (picked * weights[:, None]).reshape(frames_block.shape[0], 2, frames_block.shape[1])
    return (frames_block.astype(jnp.float32) + lax.optimization_barrier(jnp.sum(weighted, axis=1))).astype(jnp.bfloat16)

def expert_rows(slot_rows, w_up, b_up, w_down, b_down):
    preact = jnp.einsum('rd,sdf->srf', slot_rows.astype(jnp.float32), w_up.astype(jnp.float32)) + b_up[:, None, :]
    hidden = jax.nn.gelu(preact, approximate=False).astype(jnp.bfloat16)
    partial_out = jnp.einsum('srf,sfd->srd', hidden.astype(jnp.float32), w_down.astype(jnp.float32))
    rounded = lax.optimization_barrier(partial_out.astype(jnp.bfloat16)).astype(jnp.float32)
    return (lax.optimization_barrier(jnp.sum(rounded, axis=0)) + b_down).astype(jnp.bfloat16)

def reference(frames, norm_gain, norm_bias, routes, gate_codes, limits, up_weight, up_bias, down_weight, down_bias):
    blocks = N_DP * N_EXPERT
    normed = layer_norm(frames, norm_gain, norm_bias).reshape(blocks, TOK_DEV, D)

    def placer(routes_block):
        return place_slots(routes_block, limits, EXPERTS, CAP)
    slot_index, kept_mask, source_frame, filled, expert_loads = jax.vmap(placer)(routes.reshape(blocks, TOK_DEV, 2))
    sent_rows = jax.vmap(fill_slots)(normed, source_frame, filled)
    by_expert = sent_rows.reshape(blocks, EXPERTS, CAP, D).transpose(1, 0, 2, 3).reshape(EXPERTS, blocks * CAP, D)
    up_grouped = up_weight.reshape(EXPERTS, SHARDS, D, FF_DEV)
    upb_grouped = up_bias.reshape(EXPERTS, SHARDS, FF_DEV)
    down_grouped = down_weight.reshape(EXPERTS, SHARDS, FF_DEV, D)

    def one_expert(operands):
        return expert_rows(operands[0], operands[1], operands[2], operands[3], operands[4])
    outputs = lax.map(one_expert, (by_expert, up_grouped, upb_grouped, down_grouped, down_bias))
    returned = outputs.reshape(EXPERTS, blocks, CAP, D).transpose(1, 0, 2, 3).reshape(blocks, EXPERTS * CAP, D)
    mixed = jax.vmap(combine)(frames.reshape(blocks, TOK_DEV, D), returned, slot_index, kept_mask, gate_codes.reshape(blocks, TOK_DEV, 2))
    return (mixed.reshape(TOKENS, D), lax.optimization_barrier(jnp.sum(expert_loads, axis=0)).astype(jnp.int32))
```

```python
import functools
import jax
import jax.numpy as jnp
from jax import lax
from jax.experimental import pallas as pl
from jax.experimental.pallas import tpu as pltpu
from jax.sharding import PartitionSpec as P

epsilon = 1e-05
TILE = 512
PIECES = 4
CHUNKS = 2


def paired(value, step, size):
    bit = 1
    out = value
    while bit < size:
        if step & bit:
            out = out + bit - 2 * bit * lax.rem(value // bit, 2)
        bit *= 2
    return out


def moe_kernel(
    owners,
    holders,
    groups,
    capacity,
    limits,
    frames,
    gain,
    bias,
    routes,
    codes,
    up_weight,
    up_bias,
    down_weight,
    down_bias,
    mixed,
    load,
    up_all,
    down_all,
    bias_all,
    facts,
    shared,
    outgoing,
    incoming,
    hidden,
    answers,
    returned,
    halves,
    counts,
    class_count,
    group_counts,
    mix_high,
    mix_low,
    total,
    own_sem,
    weight_send,
    weight_recv,
    fact_send,
    fact_recv,
    shared_send,
    shared_recv,
    slot_send,
    slot_recv,
    back_send,
    back_recv,
    half_send,
    half_recv,
    count_send,
    count_recv,
    group_send,
    group_recv,
):
    row = lax.axis_index("dp")
    column = lax.axis_index("expert")
    near = holders // groups
    flat = row * holders + column
    place = flat // groups
    member = lax.rem(flat, groups)
    band = place // near
    spot = lax.rem(place, near)
    early = lax.rem(member, 2) == 0
    late = lax.rem(member, 2) == 1
    frame_count, width = frames.shape
    hidden_units = up_weight.shape[2]
    bands = owners // 2
    steps = owners * near
    kept_steps = bands * near
    slots = kept_steps * capacity
    block = near * capacity
    part = width // PIECES
    chunk = width // CHUNKS
    scope = jax.named_scope

    def address(expert, group):
        number = expert * groups + group
        return (number // holders, lax.rem(number, holders))

    def remote(source, target, send, recv, to):
        return pltpu.make_async_remote_copy(
            src_ref=source,
            dst_ref=target,
            send_sem=send,
            recv_sem=recv,
            device_id=to,
            device_id_type=pl.DeviceIdType.MESH,
        )

    spots = [paired(spot, j, near) for j in range(near)]
    to_band = [paired(band, k, owners) for k in range(owners)]
    ahead = [to_band[k] * near + spots[j] for k in range(owners) for j in range(near)]
    peers = [lax.rem(member + t, groups) for t in range(groups)]

    barrier = pltpu.get_barrier_semaphore()
    for r in range(1, steps):
        pl.semaphore_signal(
            barrier, inc=1, device_id=address(ahead[r], member), device_id_type=pl.DeviceIdType.MESH
        )
    for t in range(1, groups):
        pl.semaphore_signal(
            barrier, inc=1, device_id=address(place, peers[t]), device_id_type=pl.DeviceIdType.MESH
        )
    own = [
        pltpu.make_async_copy(up_weight.at[0], up_all.at[0], own_sem.at[0]),
        pltpu.make_async_copy(down_weight.at[0], down_all.at[0], own_sem.at[1]),
    ]
    for copy in own:
        copy.start()
    bias_all[0] = up_bias[...]
    facts[0, 0:2, :] = routes[...]
    facts[0, 2:4, :] = codes[...]
    facts[0, 4:8, :] = jnp.zeros((4, frame_count), jnp.int32)

    values = frames[...].astype(jnp.float32)
    center = jnp.mean(values, axis=-1, keepdims=True)
    shifted = values - center
    spread = jnp.mean(shifted * shifted, axis=-1, keepdims=True)
    normed = (shifted * lax.rsqrt(spread + epsilon) * gain[...] + bias[...]).astype(jnp.bfloat16)
    for c in range(PIECES):
        shared[0, c] = normed[:, c * part : (c + 1) * part]

    square = (frame_count, frame_count)
    across = lax.broadcasted_iota(jnp.int32, square, 1)
    along = lax.broadcasted_iota(jnp.int32, square, 0)
    earlier = jnp.where(across < along, 1.0, 0.0).astype(jnp.bfloat16)
    diagonal = across == along
    lane = lax.broadcasted_iota(jnp.int32, (1, slots), 1)
    line = lane // capacity
    slot_of = lax.rem(lane, capacity).astype(jnp.float32)

    def expert_at(q):
        return to_band[q // near] * near + q % near

    def experts(numbers):
        out = jnp.zeros(numbers.shape, jnp.int32)
        for q in range(kept_steps):
            out = jnp.where(numbers == q, expert_at(q), out)
        return out

    expert_of = experts(line)
    bound = jnp.zeros((1, slots), jnp.int32)
    for q in range(kept_steps):
        bound = jnp.where(line == q, limits[expert_at(q)], bound)
    bound = bound.astype(jnp.float32)
    tall = lax.broadcasted_iota(jnp.int32, (slots, 128), 0) // capacity
    to_lane = experts(tall) == lax.broadcasted_iota(jnp.int32, (slots, 128), 1)
    to_lane = jnp.where(to_lane, 1.0, 0.0).astype(jnp.bfloat16)

    def places(u):
        def upright(i):
            lying = facts[u, i : i + 1, :].astype(jnp.float32)
            return jnp.sum(jnp.where(diagonal, lying, 0.0), axis=1, keepdims=True)

        first, second = upright(0).astype(jnp.int32), upright(1).astype(jnp.int32)
        first_code, second_code = upright(2), upright(3)
        code_sum = first_code + second_code
        first_share, second_share = first_code / code_sum, second_code / code_sum
        hit_first, hit_second = first == expert_of, second == expert_of
        hits = jnp.where(hit_first | hit_second, 1.0, 0.0)
        rank = jnp.dot(earlier, hits.astype(jnp.bfloat16), preferred_element_type=jnp.float32)
        fits = (rank == slot_of) & (rank < bound)
        chosen = jnp.where(fits, hits, 0.0)
        picked = chosen.astype(jnp.bfloat16)
        mix = chosen * jnp.where(hit_first, first_share, second_share)
        high = mix.astype(jnp.bfloat16)
        mix_high[u] = high
        mix_low[u] = (mix - high.astype(jnp.float32)).astype(jnp.bfloat16)
        tally = jnp.dot(picked, to_lane, preferred_element_type=jnp.float32)
        return picked, jnp.sum(tally, axis=0, keepdims=True)

    def fill(u, begin, size, picked, source):
        rows = lax.dot_general(
            picked, source, (((0,), (0,)), ((), ())), preferred_element_type=jnp.float32
        )
        outgoing[u, :, :, begin : begin + size] = rows.astype(jnp.bfloat16).reshape(
            kept_steps, capacity, size
        )

    def slot_copy(u, r, c):
        k, j = r // near, r % near
        columns = pl.ds(c * part, part) if u else pl.ds(0, width)
        return remote(
            outgoing.at[u, k * near + spots[j], :, columns],
            incoming.at[u, r, :, columns],
            slot_send.at[u, r, c],
            slot_recv.at[u, r, c],
            address(ahead[r], member),
        )

    inside = list(range(1, near))
    outside = list(range(near, kept_steps))

    with scope("barrier"):
        pl.semaphore_wait(barrier, steps - 1 + groups - 1)
    other = address(to_band[bands] * near + spot, member)
    fact_copy = remote(facts.at[0], facts.at[1], fact_send, fact_recv, other)
    fact_copy.start()
    shared_copies = [
        remote(shared.at[0, c], shared.at[1, c], shared_send.at[c], shared_recv.at[c], other)
        for c in range(PIECES)
    ]

    @pl.when(early)
    def _():
        for copy in shared_copies:
            copy.start()

    weight_copies = []
    for t in range(1, groups):
        to = address(place, peers[t])
        weight_copies.append([
            remote(bias_all.at[0], bias_all.at[t], weight_send.at[t, 0], weight_recv.at[t, 0], to),
            remote(up_weight.at[0], up_all.at[t], weight_send.at[t, 1], weight_recv.at[t, 1], to),
            remote(down_weight.at[0], down_all.at[t], weight_send.at[t, 2], weight_recv.at[t, 2], to),
        ])
    for i in range(3):
        for copies in weight_copies:
            copies[i].start()

    with scope("fill0"):
        own_picks, own_tally = places(0)
        fill(0, 0, width, own_picks, normed)
    for r in inside:
        slot_copy(0, r, 0).start()
    incoming[0, 0] = outgoing[0, spot]

    @pl.when(late)
    def _():
        for r in outside:
            slot_copy(0, r, 0).start()
        with scope("slotsend"):
            for r in outside:
                slot_copy(0, r, 0).wait_send()
        for copy in shared_copies:
            copy.start()

    with scope("factwait"):
        fact_copy.wait()
    with scope("places1"):
        other_picks, other_tally = places(1)
    for c in range(PIECES):
        with scope(f"sharedwait{c}"):
            shared_copies[c].wait_recv()
        fill(1, c * part, part, other_picks, shared[1, c])
        for r in outside + inside:
            slot_copy(1, r, c).start()
    incoming[1, 0] = outgoing[1, spot]

    @pl.when(early)
    def _():
        for r in outside:
            slot_copy(0, r, 0).start()


    counts[0] = jnp.broadcast_to((own_tally + other_tally).astype(jnp.int32), (8, 128))
    count_copies = [
        remote(counts.at[0], counts.at[r], count_send.at[r], count_recv.at[r], address(ahead[r], member))
        for r in range(1, steps)
    ]
    for copy in count_copies:
        copy.start()

    out_bias = down_bias[pl.ds(place, 1), :]
    tile = min(TILE, hidden_units)

    def up(u, k, first):
        for t in range(groups):
            if first:
                with scope(f"upweight{t}"):
                    if t:
                        weight_copies[t - 1][0].wait_recv()
                        weight_copies[t - 1][1].wait_recv()
                    else:
                        own[0].wait()
            for i in range(hidden_units // tile):
                pre = jnp.dot(
                    incoming[u, pl.ds(k * near, near)].reshape(block, width),
                    up_all[t, :, i * tile : (i + 1) * tile],
                    preferred_element_type=jnp.float32,
                )
                pre = pre + bias_all[t, :, i * tile : (i + 1) * tile]
                begin = t * hidden_units + i * tile
                hidden[:, begin : begin + tile] = (
                    0.5 * pre * (1.0 + lax.erf(pre * 0.7071067811865476))
                ).astype(jnp.bfloat16)

    def back_copy(u, r, c):
        k = r // near
        columns = pl.ds(c * chunk, chunk)
        return remote(
            answers.at[u, r, :, columns],
            returned.at[u, k * near + spot, :, columns],
            back_send.at[u, r, c],
            back_recv.at[u, r, c],
            address(ahead[r], member),
        )

    def down(u, k, c):
        sums = out_bias[:, c * chunk : (c + 1) * chunk]
        for t in range(groups):
            sums = sums + jnp.dot(
                hidden[:, t * hidden_units : (t + 1) * hidden_units],
                down_all[t, :, c * chunk : (c + 1) * chunk],
                preferred_element_type=jnp.float32,
            )
        answers[u, pl.ds(k * near, near), :, c * chunk : (c + 1) * chunk] = sums.astype(
            jnp.bfloat16
        ).reshape(near, capacity, chunk)

    def arrived(u, c):
        for r in range(1, kept_steps):
            k, j = r // near, r % near
            columns = pl.ds(c * chunk, chunk)
            remote(
                answers.at[u, r, :, columns],
                returned.at[u, k * near + spots[j], :, columns],
                back_send.at[u, r, c],
                back_recv.at[u, r, c],
                address(ahead[r], member),
            ).wait_recv()

    def mixture(u, c):
        picked = returned[u, :, :, c * chunk : (c + 1) * chunk].reshape(slots, chunk)
        return jnp.dot(mix_high[u], picked, preferred_element_type=jnp.float32) + jnp.dot(
            mix_low[u], picked, preferred_element_type=jnp.float32
        )

    def rows_wait(u, k):
        for r in range(max(1, k * near), (k + 1) * near):
            for c in range(PIECES if u else 1):
                slot_copy(u, r, c).wait_recv()

    def back_start(u, k, c):
        for r in range(max(1, k * near), (k + 1) * near):
            back_copy(u, r, c).start()

    def by_member(ahead_item, behind_item, act, *more):
        if ahead_item == behind_item:
            act(*ahead_item, *more)
            return

        @pl.when(early)
        def _():
            act(*ahead_item, *more)

        @pl.when(late)
        def _():
            act(*behind_item, *more)

    far = range(1, bands)
    ahead_order = [(0, 0), (1, 0)] + [(1, k) for k in far] + [(0, k) for k in far]
    behind_order = [(0, 0)] + [(0, k) for k in far] + [(1, 0)] + [(1, k) for k in far]
    for step, (one, two) in enumerate(zip(ahead_order, behind_order)):
        u, k = (jnp.where(early, a, b) if a != b else a for a, b in zip(one, two))
        with scope(f"rows_{step}"):
            by_member(one, two, rows_wait)
        with scope(f"up_{step}"):
            up(u, k, step == 0)
        if step == 0:
            with scope("downweight"):
                own[1].wait()
                for copies in weight_copies:
                    copies[2].wait_recv()
        with scope(f"down_{step}"):
            for c in range(CHUNKS):
                down(u, k, c)
                by_member(one, two, back_start, c)
    for u in range(2):
        returned[u, spot] = answers[u, 0]

    def settle():
        for c in range(CHUNKS):
            with scope(f"arrived0{c}"):
                arrived(0, c)
            total[:, c * chunk : (c + 1) * chunk] = frames[
                :, c * chunk : (c + 1) * chunk
            ].astype(jnp.float32) + mixture(0, c)

    @pl.when(late)
    def _():
        settle()

    half_copies = [
        remote(halves.at[0, c], halves.at[1, c], half_send.at[c], half_recv.at[c], other)
        for c in range(CHUNKS)
    ]
    for c in range(CHUNKS):
        with scope(f"arrived1{c}"):
            arrived(1, c)
        halves[0, c] = mixture(1, c).astype(jnp.bfloat16)
        half_copies[c].start()

    with scope("counts"):
        for copy in count_copies:
            copy.wait()
    class_total = counts[0]
    for r in range(1, steps):
        class_total = class_total + counts[r]
    class_count[...] = class_total
    group_copies = [
        remote(class_count, group_counts.at[t], group_send.at[t], group_recv.at[t], address(place, peers[t]))
        for t in range(1, groups)
    ]
    for copy in group_copies:
        copy.start()

    @pl.when(early)
    def _():
        settle()

    with scope("groupwait"):
        for copy in group_copies:
            copy.wait()
    everything = class_count[...]
    for t in range(1, groups):
        everything = everything + group_counts[t]
    load[...] = everything

    fact_done = [copy for copies in weight_copies for copy in copies]
    for copy in fact_done:
        copy.wait_send()
    for r in inside:
        slot_copy(0, r, 0).wait_send()

    @pl.when(early)
    def _():
        for r in outside:
            slot_copy(0, r, 0).wait_send()

    for copy in shared_copies:
        copy.wait_send()

    for r in range(1, kept_steps):
        for c in range(PIECES):
            slot_copy(1, r, c).wait_send()
        for u in range(2):
            for c in range(CHUNKS):
                back_copy(u, r, c).wait_send()
    for c in range(CHUNKS):
        with scope(f"halfwait{c}"):
            half_copies[c].wait()
        mixed[:, c * chunk : (c + 1) * chunk] = (
            total[:, c * chunk : (c + 1) * chunk] + halves[1, c].astype(jnp.float32)
        ).astype(jnp.bfloat16)


def per_device(
    frames,
    norm_gain,
    norm_bias,
    routes,
    gate_codes,
    limits,
    up_weight,
    up_bias,
    down_weight,
    down_bias,
):
    owners = lax.axis_size("dp")
    holders = lax.axis_size("expert")
    expert_total = down_bias.shape[0]
    groups = owners * holders // expert_total
    frame_count, width = frames.shape
    capacity = 4 * frame_count // expert_total
    hidden_units = up_weight.shape[2]
    vmem = pl.BlockSpec(memory_space=pltpu.VMEM)
    anywhere = pl.BlockSpec(memory_space=pl.ANY)
    kept_steps = expert_total // 2
    slots = kept_steps * capacity
    blocks = (2, kept_steps, capacity, width)
    dma = pltpu.SemaphoreType.DMA
    mixed, load = pl.pallas_call(
        functools.partial(moe_kernel, owners, holders, groups, capacity),
        out_shape=(
            jax.ShapeDtypeStruct((frame_count, width), jnp.bfloat16),
            jax.ShapeDtypeStruct((8, 128), jnp.int32),
        ),
        in_specs=[
            pl.BlockSpec(memory_space=pltpu.SMEM),
            vmem,
            vmem,
            vmem,
            vmem,
            vmem,
            anywhere,
            vmem,
            anywhere,
            vmem,
        ],
        out_specs=(vmem, vmem),
        scratch_shapes=[
            pltpu.VMEM((groups, width, hidden_units), jnp.bfloat16),
            pltpu.VMEM((groups, hidden_units, width), jnp.bfloat16),
            pltpu.VMEM((groups, 1, hidden_units), jnp.float32),
            pltpu.VMEM((2, 8, frame_count), jnp.int32),
            pltpu.VMEM((2, PIECES, frame_count, width // PIECES), jnp.bfloat16),
            pltpu.VMEM(blocks, jnp.bfloat16),
            pltpu.VMEM(blocks, jnp.bfloat16),
            pltpu.VMEM((slots // (owners // 2), groups * hidden_units), jnp.bfloat16),
            pltpu.VMEM(blocks, jnp.bfloat16),
            pltpu.VMEM(blocks, jnp.bfloat16),
            pltpu.VMEM((2, CHUNKS, frame_count, width // CHUNKS), jnp.bfloat16),
            pltpu.VMEM((expert_total, 8, 128), jnp.int32),
            pltpu.VMEM((8, 128), jnp.int32),
            pltpu.VMEM((groups, 8, 128), jnp.int32),
            pltpu.VMEM((2, frame_count, slots), jnp.bfloat16),
            pltpu.VMEM((2, frame_count, slots), jnp.bfloat16),
            pltpu.VMEM((frame_count, width), jnp.float32),
            dma((2,)),
            dma((groups, 3)),
            dma((groups, 3)),
            dma(()),
            dma(()),
            dma((PIECES,)),
            dma((PIECES,)),
            dma((2, kept_steps, PIECES)),
            dma((2, kept_steps, PIECES)),
            dma((2, kept_steps, CHUNKS)),
            dma((2, kept_steps, CHUNKS)),
            dma((CHUNKS,)),
            dma((CHUNKS,)),
            dma((expert_total,)),
            dma((expert_total,)),
            dma((groups,)),
            dma((groups,)),
        ],
        compiler_params=pltpu.CompilerParams(
            collective_id=0, has_side_effects=True, vmem_limit_bytes=56 * 1024 * 1024
        ),
        name="moe",
    )(
        limits,
        frames,
        norm_gain.reshape(1, width),
        norm_bias.reshape(1, width),
        routes.T,
        gate_codes.T,
        up_weight,
        up_bias,
        down_weight,
        down_bias,
    )
    return (mixed, load[0, :expert_total])


def solution(mesh):
    in_specs = (
        P(("dp", "expert"), None),
        P(),
        P(),
        P(("dp", "expert"), None),
        P(("dp", "expert"), None),
        P(),
        P(("dp", "expert"), None, None),
        P(("dp", "expert"), None),
        P(("dp", "expert"), None, None),
        P(),
    )
    out_specs = (P(("dp", "expert"), None), P())
    return jax.shard_map(
        per_device, mesh=mesh, in_specs=in_specs, out_specs=out_specs, check_vma=False
    )
```

```python
import functools
import jax
import jax.numpy as jnp
from jax import lax
from jax.experimental import pallas as pl
from jax.experimental.pallas import tpu as pltpu
from jax.sharding import PartitionSpec as P

epsilon = 1e-05
TILE = 512
PIECES = 4
CHUNKS = 2


def paired(value, step, size):
    bit = 1
    out = value
    while bit < size:
        if step & bit:
            out = out + bit - 2 * bit * lax.rem(value // bit, 2)
        bit *= 2
    return out


def moe_kernel(
    owners,
    holders,
    groups,
    capacity,
    limits,
    frames,
    gain,
    bias,
    routes,
    codes,
    up_weight,
    up_bias,
    down_weight,
    down_bias,
    mixed,
    load,
    up_all,
    down_all,
    bias_all,
    facts,
    shared,
    outgoing,
    incoming,
    hidden,
    answers,
    returned,
    halves,
    counts,
    class_count,
    group_counts,
    mix_high,
    mix_low,
    total,
    own_sem,
    weight_send,
    weight_recv,
    fact_send,
    fact_recv,
    shared_send,
    shared_recv,
    slot_send,
    slot_recv,
    back_send,
    back_recv,
    half_send,
    half_recv,
    count_send,
    count_recv,
    group_send,
    group_recv,
):
    row = lax.axis_index("dp")
    column = lax.axis_index("expert")
    near = holders // groups
    flat = row * holders + column
    place = flat // groups
    member = lax.rem(flat, groups)
    band = place // near
    spot = lax.rem(place, near)
    early = lax.rem(member, 2) == 0
    late = lax.rem(member, 2) == 1
    frame_count, width = frames.shape
    hidden_units = up_weight.shape[2]
    bands = owners // 2
    steps = owners * near
    kept_steps = bands * near
    slots = kept_steps * capacity
    block = near * capacity
    part = width // PIECES
    chunk = width // CHUNKS
    scope = jax.named_scope

    def address(expert, group):
        number = expert * groups + group
        return (number // holders, lax.rem(number, holders))

    def remote(source, target, send, recv, to):
        return pltpu.make_async_remote_copy(
            src_ref=source,
            dst_ref=target,
            send_sem=send,
            recv_sem=recv,
            device_id=to,
            device_id_type=pl.DeviceIdType.MESH,
        )

    spots = [paired(spot, j, near) for j in range(near)]
    to_band = [paired(band, k, owners) for k in range(owners)]
    ahead = [to_band[k] * near + spots[j] for k in range(owners) for j in range(near)]
    peers = [lax.rem(member + t, groups) for t in range(groups)]

    barrier = pltpu.get_barrier_semaphore()
    for r in range(1, steps):
        pl.semaphore_signal(
            barrier, inc=1, device_id=address(ahead[r], member), device_id_type=pl.DeviceIdType.MESH
        )
    for t in range(1, groups):
        pl.semaphore_signal(
            barrier, inc=1, device_id=address(place, peers[t]), device_id_type=pl.DeviceIdType.MESH
        )
    own = [
        pltpu.make_async_copy(up_weight.at[0], up_all.at[0], own_sem.at[0]),
        pltpu.make_async_copy(down_weight.at[0], down_all.at[0], own_sem.at[1]),
    ]
    for copy in own:
        copy.start()
    bias_all[0] = up_bias[...]
    facts[0, 0:2, :] = routes[...]
    facts[0, 2:4, :] = codes[...]
    facts[0, 4:8, :] = jnp.zeros((4, frame_count), jnp.int32)

    values = frames[...].astype(jnp.float32)
    center = jnp.mean(values, axis=-1, keepdims=True)
    shifted = values - center
    spread = jnp.mean(shifted * shifted, axis=-1, keepdims=True)
    normed = (shifted * lax.rsqrt(spread + epsilon) * gain[...] + bias[...]).astype(jnp.bfloat16)
    for c in range(PIECES):
        shared[0, c] = normed[:, c * part : (c + 1) * part]

    square = (frame_count, frame_count)
    across = lax.broadcasted_iota(jnp.int32, square, 1)
    along = lax.broadcasted_iota(jnp.int32, square, 0)
    earlier = jnp.where(across < along, 1.0, 0.0).astype(jnp.bfloat16)
    diagonal = across == along
    lane = lax.broadcasted_iota(jnp.int32, (1, slots), 1)
    line = lane // capacity
    slot_of = lax.rem(lane, capacity).astype(jnp.float32)

    def expert_at(q):
        return to_band[q // near] * near + q % near

    def experts(numbers):
        out = jnp.zeros(numbers.shape, jnp.int32)
        for q in range(kept_steps):
            out = jnp.where(numbers == q, expert_at(q), out)
        return out

    expert_of = experts(line)
    bound = jnp.zeros((1, slots), jnp.int32)
    for q in range(kept_steps):
        bound = jnp.where(line == q, limits[expert_at(q)], bound)
    bound = bound.astype(jnp.float32)
    tall = lax.broadcasted_iota(jnp.int32, (slots, 128), 0) // capacity
    to_lane = experts(tall) == lax.broadcasted_iota(jnp.int32, (slots, 128), 1)
    to_lane = jnp.where(to_lane, 1.0, 0.0).astype(jnp.bfloat16)

    def places(u):
        def upright(i):
            lying = facts[u, i : i + 1, :].astype(jnp.float32)
            return jnp.sum(jnp.where(diagonal, lying, 0.0), axis=1, keepdims=True)

        first, second = upright(0).astype(jnp.int32), upright(1).astype(jnp.int32)
        first_code, second_code = upright(2), upright(3)
        code_sum = first_code + second_code
        first_share, second_share = first_code / code_sum, second_code / code_sum
        hit_first, hit_second = first == expert_of, second == expert_of
        hits = jnp.where(hit_first | hit_second, 1.0, 0.0)
        rank = jnp.dot(earlier, hits.astype(jnp.bfloat16), preferred_element_type=jnp.float32)
        fits = (rank == slot_of) & (rank < bound)
        chosen = jnp.where(fits, hits, 0.0)
        picked = chosen.astype(jnp.bfloat16)
        mix = chosen * jnp.where(hit_first, first_share, second_share)
        high = mix.astype(jnp.bfloat16)
        mix_high[u] = high
        mix_low[u] = (mix - high.astype(jnp.float32)).astype(jnp.bfloat16)
        tally = jnp.dot(picked, to_lane, preferred_element_type=jnp.float32)
        return picked, jnp.sum(tally, axis=0, keepdims=True)

    def fill(u, begin, size, picked, source):
        rows = lax.dot_general(
            picked, source, (((0,), (0,)), ((), ())), preferred_element_type=jnp.float32
        )
        outgoing[u, :, :, begin : begin + size] = rows.astype(jnp.bfloat16).reshape(
            kept_steps, capacity, size
        )

    def slot_copy(u, r, c):
        k, j = r // near, r % near
        columns = pl.ds(c * part, part) if u else pl.ds(0, width)
        return remote(
            outgoing.at[u, k * near + spots[j], :, columns],
            incoming.at[u, r, :, columns],
            slot_send.at[u, r, c],
            slot_recv.at[u, r, c],
            address(ahead[r], member),
        )

    inside = list(range(1, near))
    outside = list(range(near, kept_steps))

    with scope("barrier"):
        pl.semaphore_wait(barrier, steps - 1 + groups - 1)
    other = address(to_band[bands] * near + spot, member)
    fact_copy = remote(facts.at[0], facts.at[1], fact_send, fact_recv, other)
    fact_copy.start()
    shared_copies = [
        remote(shared.at[0, c], shared.at[1, c], shared_send.at[c], shared_recv.at[c], other)
        for c in range(PIECES)
    ]

    @pl.when(early)
    def _():
        for copy in shared_copies:
            copy.start()

    weight_copies = []
    for t in range(1, groups):
        to = address(place, peers[t])
        weight_copies.append([
            remote(bias_all.at[0], bias_all.at[t], weight_send.at[t, 0], weight_recv.at[t, 0], to),
            remote(up_weight.at[0], up_all.at[t], weight_send.at[t, 1], weight_recv.at[t, 1], to),
            remote(down_weight.at[0], down_all.at[t], weight_send.at[t, 2], weight_recv.at[t, 2], to),
        ])
    for i in range(3):
        for copies in weight_copies:
            copies[i].start()

    with scope("fill0"):
        own_picks, own_tally = places(0)
        fill(0, 0, width, own_picks, normed)
    for r in inside:
        slot_copy(0, r, 0).start()
    incoming[0, 0] = outgoing[0, spot]

    @pl.when(late)
    def _():
        for r in outside:
            slot_copy(0, r, 0).start()
        with scope("slotsend"):
            for r in outside:
                slot_copy(0, r, 0).wait_send()
        for copy in shared_copies:
            copy.start()

    with scope("factwait"):
        fact_copy.wait()
    with scope("places1"):
        other_picks, other_tally = places(1)
    counts[0] = jnp.broadcast_to((own_tally + other_tally).astype(jnp.int32), (8, 128))
    count_copies = [
        remote(counts.at[0], counts.at[r], count_send.at[r], count_recv.at[r], address(ahead[r], member))
        for r in range(1, steps)
    ]
    for copy in count_copies:
        copy.start()

    def pass_on(c):
        with scope(f"sharedwait{c}"):
            shared_copies[c].wait_recv()
        fill(1, c * part, part, other_picks, shared[1, c])
        for r in inside + outside:
            slot_copy(1, r, c).start()

    out_bias = down_bias[pl.ds(place, 1), :]
    tile = min(TILE, hidden_units)

    def up(u, k, at, first):
        for t in range(groups):
            if first:
                with scope(f"upweight{t}"):
                    if t:
                        weight_copies[t - 1][0].wait_recv()
                        weight_copies[t - 1][1].wait_recv()
                    else:
                        own[0].wait()
            for i in range(hidden_units // tile):
                pre = jnp.dot(
                    incoming[u, pl.ds(k * near, near)].reshape(block, width),
                    up_all[t, :, i * tile : (i + 1) * tile],
                    preferred_element_type=jnp.float32,
                )
                pre = pre + bias_all[t, :, i * tile : (i + 1) * tile]
                begin = t * hidden_units + i * tile
                hidden[at, :, begin : begin + tile] = (
                    0.5 * pre * (1.0 + lax.erf(pre * 0.7071067811865476))
                ).astype(jnp.bfloat16)

    def back_copy(u, r, c):
        k = r // near
        columns = pl.ds(c * chunk, chunk)
        return remote(
            answers.at[u, r, :, columns],
            returned.at[u, k * near + spot, :, columns],
            back_send.at[u, r, c],
            back_recv.at[u, r, c],
            address(ahead[r], member),
        )

    def down(u, k, at, c):
        sums = out_bias[:, c * chunk : (c + 1) * chunk]
        for t in range(groups):
            sums = sums + jnp.dot(
                hidden[at, :, t * hidden_units : (t + 1) * hidden_units],
                down_all[t, :, c * chunk : (c + 1) * chunk],
                preferred_element_type=jnp.float32,
            )
        answers[u, pl.ds(k * near, near), :, c * chunk : (c + 1) * chunk] = sums.astype(
            jnp.bfloat16
        ).reshape(near, capacity, chunk)

    def arrived(u, c):
        for r in range(1, kept_steps):
            k, j = r // near, r % near
            columns = pl.ds(c * chunk, chunk)
            remote(
                answers.at[u, r, :, columns],
                returned.at[u, k * near + spots[j], :, columns],
                back_send.at[u, r, c],
                back_recv.at[u, r, c],
                address(ahead[r], member),
            ).wait_recv()

    def mixture(u, c):
        picked = returned[u, :, :, c * chunk : (c + 1) * chunk].reshape(slots, chunk)
        return jnp.dot(mix_high[u], picked, preferred_element_type=jnp.float32) + jnp.dot(
            mix_low[u], picked, preferred_element_type=jnp.float32
        )

    def rows_wait(u, k):
        for r in range(max(1, k * near), (k + 1) * near):
            for c in range(PIECES if u else 1):
                slot_copy(u, r, c).wait_recv()

    def back_start(u, k, c):
        for r in range(max(1, k * near), (k + 1) * near):
            back_copy(u, r, c).start()

    def by_member(one, two, act):
        if one == two:
            act(one)
            return
        for item, mine in ((one, early), (two, late)):
            if item is not None:
                pl.when(mine)(functools.partial(act, item))

    def both(one, two):
        return [a if a == b else jnp.where(early, a, b) for a, b in zip(one, two)]

    def rise(one, two):
        def act(item):
            with scope(f"up_{item[0]}{item[1]}"):
                up(*item, False)

        def rows(item):
            with scope(f"rows_{item[0]}{item[1]}"):
                rows_wait(item[0], item[1])

        by_member(one, two, rows)
        if one is None or two is None:
            by_member(one, two, act)
        else:
            with scope("up"):
                up(*both(one, two), one == two)

    def fall(one, two):
        for c in range(CHUNKS):
            if one is None or two is None:
                by_member(one, two, lambda item: down(*item, c))
            else:
                with scope(f"down{c}"):
                    down(*both(one, two), c)
            by_member(one, two, lambda item: back_start(item[0], item[1], c))

    def down_weights():
        with scope("downweight"):
            own[1].wait()
            for copies in weight_copies:
                copies[2].wait_recv()

    def pass_all():
        for c in range(PIECES):
            pass_on(c)
        incoming[1, 0] = outgoing[1, spot]

    far = list(range(1, bands))
    pl.when(early)(pass_all)
    rise((0, 0, 0), (0, 0, 0))
    rise((1, 0, 1), (0, 1, 1))
    for k in far[1:]:
        rise(None, (0, k, k))

    @pl.when(early)
    def _():
        for r in outside:
            slot_copy(0, r, 0).start()

    @pl.when(late)
    def _():
        pass_all()
        down_weights()

    fall(None, (0, 0, 0))
    rise((1, 1, bands), (1, 0, 0))
    for k in far[1:]:
        rise((1, k, bands - 1 + k), (1, k - 1, bands - 2 + k))
    rise(None, (1, bands - 1, 2 * bands - 2))
    pl.when(early)(down_weights)
    for k in far:
        fall((1, k, bands - 1 + k), (1, k, bands - 1 + k))
    fall((1, 0, 1), (1, 0, 0))
    returned[1, spot] = answers[1, 0]
    fall((0, 0, 0), (0, 1, 1))
    for k in far[1:]:
        fall(None, (0, k, k))
    returned[0, spot] = answers[0, 0]

    half_copies = [
        remote(halves.at[0, c], halves.at[1, c], half_send.at[c], half_recv.at[c], other)
        for c in range(CHUNKS)
    ]
    for c in range(CHUNKS):
        with scope(f"arrived1{c}"):
            arrived(1, c)
        halves[0, c] = mixture(1, c).astype(jnp.bfloat16)
        half_copies[c].start()

    for k in far:
        rise((0, k, 0), None)
        fall((0, k, 0), None)

    with scope("counts"):
        for copy in count_copies:
            copy.wait()
    class_total = counts[0]
    for r in range(1, steps):
        class_total = class_total + counts[r]
    class_count[...] = class_total
    group_copies = [
        remote(class_count, group_counts.at[t], group_send.at[t], group_recv.at[t], address(place, peers[t]))
        for t in range(1, groups)
    ]
    for copy in group_copies:
        copy.start()

    for c in range(CHUNKS):
        with scope(f"arrived0{c}"):
            arrived(0, c)
        total[:, c * chunk : (c + 1) * chunk] = frames[:, c * chunk : (c + 1) * chunk].astype(
            jnp.float32
        ) + mixture(0, c)
    with scope("groupwait"):
        for copy in group_copies:
            copy.wait()
    everything = class_count[...]
    for t in range(1, groups):
        everything = everything + group_counts[t]
    load[...] = everything

    fact_done = [copy for copies in weight_copies for copy in copies]
    for copy in fact_done:
        copy.wait_send()
    for r in inside:
        slot_copy(0, r, 0).wait_send()

    @pl.when(early)
    def _():
        for r in outside:
            slot_copy(0, r, 0).wait_send()

    for copy in shared_copies:
        copy.wait_send()

    for r in range(1, kept_steps):
        for c in range(PIECES):
            slot_copy(1, r, c).wait_send()
        for u in range(2):
            for c in range(CHUNKS):
                back_copy(u, r, c).wait_send()
    for c in range(CHUNKS):
        with scope(f"halfwait{c}"):
            half_copies[c].wait()
        mixed[:, c * chunk : (c + 1) * chunk] = (
            total[:, c * chunk : (c + 1) * chunk] + halves[1, c].astype(jnp.float32)
        ).astype(jnp.bfloat16)


def finish_kernel(mixed, load, mixed_out, load_out):
    mixed_out[...] = mixed[...]
    load_out[...] = load[0:1, 0 : load_out.shape[1]]


def per_device(
    frames,
    norm_gain,
    norm_bias,
    routes,
    gate_codes,
    limits,
    up_weight,
    up_bias,
    down_weight,
    down_bias,
):
    owners = lax.axis_size("dp")
    holders = lax.axis_size("expert")
    expert_total = down_bias.shape[0]
    groups = owners * holders // expert_total
    frame_count, width = frames.shape
    capacity = 4 * frame_count // expert_total
    hidden_units = up_weight.shape[2]
    vmem = pl.BlockSpec(memory_space=pltpu.VMEM)
    anywhere = pl.BlockSpec(memory_space=pl.ANY)
    kept_steps = expert_total // 2
    slots = kept_steps * capacity
    blocks = (2, kept_steps, capacity, width)
    dma = pltpu.SemaphoreType.DMA
    mixed, load = pl.pallas_call(
        functools.partial(moe_kernel, owners, holders, groups, capacity),
        out_shape=(
            pltpu.VMEM((frame_count, width), jnp.bfloat16),
            pltpu.VMEM((8, 128), jnp.int32),
        ),
        in_specs=[
            pl.BlockSpec(memory_space=pltpu.SMEM),
            vmem,
            vmem,
            vmem,
            vmem,
            vmem,
            anywhere,
            vmem,
            anywhere,
            vmem,
        ],
        out_specs=(vmem, vmem),
        scratch_shapes=[
            pltpu.VMEM((groups, width, hidden_units), jnp.bfloat16),
            pltpu.VMEM((groups, hidden_units, width), jnp.bfloat16),
            pltpu.VMEM((groups, 1, hidden_units), jnp.float32),
            pltpu.VMEM((2, 8, frame_count), jnp.int32),
            pltpu.VMEM((2, PIECES, frame_count, width // PIECES), jnp.bfloat16),
            pltpu.VMEM(blocks, jnp.bfloat16),
            pltpu.VMEM(blocks, jnp.bfloat16),
            pltpu.VMEM((owners - 1, slots // (owners // 2), groups * hidden_units), jnp.bfloat16),
            pltpu.VMEM(blocks, jnp.bfloat16),
            pltpu.VMEM(blocks, jnp.bfloat16),
            pltpu.VMEM((2, CHUNKS, frame_count, width // CHUNKS), jnp.bfloat16),
            pltpu.VMEM((expert_total, 8, 128), jnp.int32),
            pltpu.VMEM((8, 128), jnp.int32),
            pltpu.VMEM((groups, 8, 128), jnp.int32),
            pltpu.VMEM((2, frame_count, slots), jnp.bfloat16),
            pltpu.VMEM((2, frame_count, slots), jnp.bfloat16),
            pltpu.VMEM((frame_count, width), jnp.float32),
            dma((2,)),
            dma((groups, 3)),
            dma((groups, 3)),
            dma(()),
            dma(()),
            dma((PIECES,)),
            dma((PIECES,)),
            dma((2, kept_steps, PIECES)),
            dma((2, kept_steps, PIECES)),
            dma((2, kept_steps, CHUNKS)),
            dma((2, kept_steps, CHUNKS)),
            dma((CHUNKS,)),
            dma((CHUNKS,)),
            dma((expert_total,)),
            dma((expert_total,)),
            dma((groups,)),
            dma((groups,)),
        ],
        compiler_params=pltpu.CompilerParams(
            collective_id=0, has_side_effects=True, vmem_limit_bytes=56 * 1024 * 1024
        ),
        name="moe",
    )(
        limits,
        frames,
        norm_gain.reshape(1, width),
        norm_bias.reshape(1, width),
        routes.T,
        gate_codes.T,
        up_weight,
        up_bias,
        down_weight,
        down_bias,
    )
    mixed, load = pl.pallas_call(
        finish_kernel,
        out_shape=(
            jax.ShapeDtypeStruct((frame_count, width), jnp.bfloat16),
            jax.ShapeDtypeStruct((1, expert_total), jnp.int32),
        ),
        in_specs=[vmem, vmem],
        out_specs=(vmem, vmem),
        compiler_params=pltpu.CompilerParams(vmem_limit_bytes=2 * 1024 * 1024),
        name="finish",
    )(mixed, load)
    return (mixed, load.reshape(expert_total))


def solution(mesh):
    in_specs = (
        P(("dp", "expert"), None),
        P(),
        P(),
        P(("dp", "expert"), None),
        P(("dp", "expert"), None),
        P(),
        P(("dp", "expert"), None, None),
        P(("dp", "expert"), None),
        P(("dp", "expert"), None, None),
        P(),
    )
    out_specs = (P(("dp", "expert"), None), P())
    return jax.shard_map(
        per_device, mesh=mesh, in_specs=in_specs, out_specs=out_specs, check_vma=False
    )
```

```python
import functools
import jax
import jax.numpy as jnp
from jax import lax
from jax.experimental import pallas as pl
from jax.experimental.pallas import tpu as pltpu
from jax.sharding import PartitionSpec as P

epsilon = 1e-05
TILE = 512
PIECES = 4
CHUNKS = 4
WIDE = 2


def paired(value, step, size):
    bit = 1
    out = value
    while bit < size:
        if step & bit:
            out = out + bit - 2 * bit * lax.rem(value // bit, 2)
        bit *= 2
    return out


def moe_kernel(
    owners,
    holders,
    groups,
    capacity,
    limits_in,
    frames_in,
    gain_in,
    bias_in,
    routes_in,
    codes_in,
    up_weight,
    up_bias,
    down_weight,
    down_bias_in,
    mixed,
    load,
    limits,
    frames,
    gain,
    bias,
    routes,
    codes,
    down_bias,
    up_all,
    down_all,
    bias_all,
    facts,
    shared,
    outgoing,
    incoming,
    hidden,
    answers,
    returned,
    halves,
    counts,
    half_counts,
    class_count,
    group_counts,
    mix_high,
    mix_low,
    total,
    load_sem,
    own_sem,
    weight_send,
    weight_recv,
    fact_send,
    fact_recv,
    shared_send,
    shared_recv,
    slot_send,
    slot_recv,
    back_send,
    back_recv,
    half_send,
    half_recv,
    count_send,
    count_recv,
    pair_send,
    pair_recv,
    group_send,
    group_recv,
):
    row = lax.axis_index("dp")
    column = lax.axis_index("expert")
    near = holders // groups
    flat = row * holders + column
    place = flat // groups
    member = lax.rem(flat, groups)
    band = place // near
    spot = lax.rem(place, near)
    early = lax.rem(member, 2) == 0
    late = lax.rem(member, 2) == 1
    frame_count, width = frames.shape
    hidden_units = up_weight.shape[2]
    bands = owners // 2
    kept_steps = bands * near
    slots = kept_steps * capacity
    block = near * capacity
    part = width // PIECES
    chunk = width // CHUNKS
    scope = jax.named_scope

    def address(expert, group):
        number = expert * groups + group
        return (number // holders, lax.rem(number, holders))

    def remote(source, target, send, recv, to):
        return pltpu.make_async_remote_copy(
            src_ref=source,
            dst_ref=target,
            send_sem=send,
            recv_sem=recv,
            device_id=to,
            device_id_type=pl.DeviceIdType.MESH,
        )

    spots = [paired(spot, j, near) for j in range(near)]
    to_band = [paired(band, k, owners) for k in range(owners)]
    ahead = [to_band[k] * near + spots[j] for k in range(owners) for j in range(near)]
    peers = [lax.rem(member + t, groups) for t in range(groups)]

    barrier = pltpu.get_barrier_semaphore()
    other = address(to_band[bands] * near + spot, member)
    pl.semaphore_signal(barrier, inc=1, device_id=other, device_id_type=pl.DeviceIdType.MESH)
    for r in range(1, kept_steps):
        pl.semaphore_signal(
            barrier, inc=1, device_id=address(ahead[r], member), device_id_type=pl.DeviceIdType.MESH
        )
    for t in range(1, groups):
        pl.semaphore_signal(
            barrier, inc=1, device_id=address(place, peers[t]), device_id_type=pl.DeviceIdType.MESH
        )
    loads = [
        pltpu.make_async_copy(source, target, load_sem.at[i])
        for i, (source, target) in enumerate(
            (
                (frames_in, frames),
                (gain_in, gain),
                (bias_in, bias),
                (routes_in, routes),
                (codes_in, codes),
                (limits_in, limits),
                (up_bias, bias_all.at[0]),
                (down_bias_in, down_bias),
            )
        )
    ]
    for copy in loads:
        copy.start()
    own = [
        pltpu.make_async_copy(up_weight.at[0], up_all.at[0], own_sem.at[0]),
        pltpu.make_async_copy(down_weight.at[0], down_all.at[0], own_sem.at[1]),
    ]
    for copy in loads[:3]:
        copy.wait()

    values = frames[...].astype(jnp.float32)
    center = jnp.mean(values, axis=-1, keepdims=True)
    shifted = values - center
    spread = jnp.mean(shifted * shifted, axis=-1, keepdims=True)
    normed = (shifted * lax.rsqrt(spread + epsilon) * gain[...] + bias[...]).astype(jnp.bfloat16)
    for c in range(PIECES):
        shared[0, c] = normed[:, c * part : (c + 1) * part]
    for copy in loads[3:]:
        copy.wait()
    facts[0, 0:2, :] = routes[...]
    facts[0, 2:4, :] = codes[...]
    facts[0, 4:8, :] = jnp.zeros((4, frame_count), jnp.int32)
    for copy in own:
        copy.start()

    square = (frame_count, frame_count)
    across = lax.broadcasted_iota(jnp.int32, square, 1)
    along = lax.broadcasted_iota(jnp.int32, square, 0)
    earlier = jnp.where(across < along, 1.0, 0.0).astype(jnp.bfloat16)
    diagonal = across == along
    lane = lax.broadcasted_iota(jnp.int32, (1, slots), 1)
    line = lane // capacity
    slot_of = lax.rem(lane, capacity).astype(jnp.float32)

    def expert_at(q):
        return to_band[q // near] * near + q % near

    def experts(numbers):
        out = jnp.zeros(numbers.shape, jnp.int32)
        for q in range(kept_steps):
            out = jnp.where(numbers == q, expert_at(q), out)
        return out

    expert_of = experts(line)
    bound = jnp.zeros((1, slots), jnp.int32)
    for q in range(kept_steps):
        bound = jnp.where(line == q, limits[expert_at(q)], bound)
    bound = bound.astype(jnp.float32)
    tall = lax.broadcasted_iota(jnp.int32, (slots, 128), 0) // capacity
    to_lane = experts(tall) == lax.broadcasted_iota(jnp.int32, (slots, 128), 1)
    to_lane = jnp.where(to_lane, 1.0, 0.0).astype(jnp.bfloat16)

    def places(u):
        def upright(i):
            lying = facts[u, i : i + 1, :].astype(jnp.float32)
            return jnp.sum(jnp.where(diagonal, lying, 0.0), axis=1, keepdims=True)

        first, second = upright(0).astype(jnp.int32), upright(1).astype(jnp.int32)
        first_code, second_code = upright(2), upright(3)
        code_sum = first_code + second_code
        first_share, second_share = first_code / code_sum, second_code / code_sum
        hit_first, hit_second = first == expert_of, second == expert_of
        hits = jnp.where(hit_first | hit_second, 1.0, 0.0)
        rank = jnp.dot(earlier, hits.astype(jnp.bfloat16), preferred_element_type=jnp.float32)
        fits = (rank == slot_of) & (rank < bound)
        chosen = jnp.where(fits, hits, 0.0)
        picked = chosen.astype(jnp.bfloat16)
        mix = chosen * jnp.where(hit_first, first_share, second_share)
        high = mix.astype(jnp.bfloat16)
        mix_high[u] = high
        mix_low[u] = (mix - high.astype(jnp.float32)).astype(jnp.bfloat16)
        tally = jnp.dot(picked, to_lane, preferred_element_type=jnp.float32)
        return picked, jnp.sum(tally, axis=0, keepdims=True)

    def fill(u, begin, size, picked, source):
        rows = lax.dot_general(
            picked, source, (((0,), (0,)), ((), ())), preferred_element_type=jnp.float32
        )
        outgoing[u, :, :, begin : begin + size] = rows.astype(jnp.bfloat16).reshape(
            kept_steps, capacity, size
        )

    def slot_copy(u, r, c):
        k, j = r // near, r % near
        columns = pl.ds(c * part, part) if u else pl.ds(0, width)
        return remote(
            outgoing.at[u, k * near + spots[j], :, columns],
            incoming.at[u, r, :, columns],
            slot_send.at[u, r, c],
            slot_recv.at[u, r, c],
            address(ahead[r], member),
        )

    inside = list(range(1, near))
    outside = list(range(near, kept_steps))

    with scope("barrier"):
        pl.semaphore_wait(barrier, kept_steps + groups - 1)
    fact_copy = remote(facts.at[0], facts.at[1], fact_send, fact_recv, other)
    fact_copy.start()
    shared_copies = [
        remote(shared.at[0, c], shared.at[1, c], shared_send.at[c], shared_recv.at[c], other)
        for c in range(PIECES)
    ]

    @pl.when(early)
    def _():
        for copy in shared_copies:
            copy.start()

    weight_copies = []
    for t in range(1, groups):
        to = address(place, peers[t])
        weight_copies.append([
            remote(bias_all.at[0], bias_all.at[t], weight_send.at[t, 0], weight_recv.at[t, 0], to),
            remote(up_weight.at[0], up_all.at[t], weight_send.at[t, 1], weight_recv.at[t, 1], to),
            remote(down_weight.at[0], down_all.at[t], weight_send.at[t, 2], weight_recv.at[t, 2], to),
        ])
    for i in range(3):
        for copies in weight_copies:
            copies[i].start()

    with scope("fill0"):
        own_picks, own_tally = places(0)
        fill(0, 0, width, own_picks, normed)
    for r in inside:
        slot_copy(0, r, 0).start()
    incoming[0, 0] = outgoing[0, spot]

    @pl.when(late)
    def _():
        for r in outside:
            slot_copy(0, r, 0).start()
        with scope("slotsend"):
            for r in outside:
                slot_copy(0, r, 0).wait_send()
        for copy in shared_copies:
            copy.start()

    with scope("factwait"):
        fact_copy.wait()
    with scope("places1"):
        other_picks, other_tally = places(1)
    counts[0] = jnp.broadcast_to((own_tally + other_tally).astype(jnp.int32), (8, 128))
    count_copies = [
        remote(counts.at[0], counts.at[r], count_send.at[r], count_recv.at[r], address(ahead[r], member))
        for r in range(1, kept_steps)
    ]
    for copy in count_copies:
        copy.start()

    def pass_on(c):
        with scope(f"sharedwait{c}"):
            shared_copies[c].wait_recv()
        fill(1, c * part, part, other_picks, shared[1, c])
        for r in inside + outside:
            slot_copy(1, r, c).start()

    out_bias = down_bias[pl.ds(place, 1), :]
    tile = min(TILE, hidden_units)

    def up(u, k, at, first):
        for t in range(groups):
            if first:
                with scope(f"upweight{t}"):
                    if t:
                        weight_copies[t - 1][0].wait_recv()
                        weight_copies[t - 1][1].wait_recv()
                    else:
                        own[0].wait()
            for i in range(hidden_units // tile):
                pre = jnp.dot(
                    incoming[u, pl.ds(k * near, near)].reshape(block, width),
                    up_all[t, :, i * tile : (i + 1) * tile],
                    preferred_element_type=jnp.float32,
                )
                pre = pre + bias_all[t, :, i * tile : (i + 1) * tile]
                begin = t * hidden_units + i * tile
                hidden[at, :, begin : begin + tile] = (
                    0.5 * pre * (1.0 + lax.erf(pre * 0.7071067811865476))
                ).astype(jnp.bfloat16)

    def back_copy(u, r, c):
        k = r // near
        columns = pl.ds(c * chunk, chunk)
        return remote(
            answers.at[u, r, :, columns],
            returned.at[u, k * near + spot, :, columns],
            back_send.at[u, r, c],
            back_recv.at[u, r, c],
            address(ahead[r], member),
        )

    def down(u, k, at, c):
        begin, end = c * width // WIDE, (c + 1) * width // WIDE
        sums = out_bias[:, begin:end]
        for t in range(groups):
            sums = sums + jnp.dot(
                hidden[at, :, t * hidden_units : (t + 1) * hidden_units],
                down_all[t, :, begin:end],
                preferred_element_type=jnp.float32,
            )
        answers[u, pl.ds(k * near, near), :, begin:end] = sums.astype(jnp.bfloat16).reshape(
            near, capacity, end - begin
        )

    def arrived(u, c):
        for r in range(1, kept_steps):
            k, j = r // near, r % near
            columns = pl.ds(c * chunk, chunk)
            remote(
                answers.at[u, r, :, columns],
                returned.at[u, k * near + spots[j], :, columns],
                back_send.at[u, r, c],
                back_recv.at[u, r, c],
                address(ahead[r], member),
            ).wait_recv()

    def mixture(u, c):
        picked = returned[u, :, :, c * chunk : (c + 1) * chunk].reshape(slots, chunk)
        return jnp.dot(mix_high[u], picked, preferred_element_type=jnp.float32) + jnp.dot(
            mix_low[u], picked, preferred_element_type=jnp.float32
        )

    def rows_wait(u, k):
        for r in range(max(1, k * near), (k + 1) * near):
            for c in range(PIECES if u else 1):
                slot_copy(u, r, c).wait_recv()

    def back_start(u, k, c):
        for r in range(max(1, k * near), (k + 1) * near):
            back_copy(u, r, c).start()

    def by_member(one, two, act):
        if one == two:
            act(one)
            return
        for item, mine in ((one, early), (two, late)):
            if item is not None:
                pl.when(mine)(functools.partial(act, item))

    def both(one, two):
        return [a if a == b else jnp.where(early, a, b) for a, b in zip(one, two)]

    def rise(one, two):
        def act(item):
            with scope(f"up_{item[0]}{item[1]}"):
                up(*item, False)

        def rows(item):
            with scope(f"rows_{item[0]}{item[1]}"):
                rows_wait(item[0], item[1])

        by_member(one, two, rows)
        if one is None or two is None:
            by_member(one, two, act)
        else:
            with scope("up"):
                up(*both(one, two), one == two)

    def fall(one, two):
        for w in range(WIDE):
            if one is None or two is None:
                by_member(one, two, lambda item: down(*item, w))
            else:
                with scope(f"down{w}"):
                    down(*both(one, two), w)
            for c in range(w * CHUNKS // WIDE, (w + 1) * CHUNKS // WIDE):
                by_member(one, two, lambda item: back_start(item[0], item[1], c))

    def down_weights():
        with scope("downweight"):
            own[1].wait()
            for copies in weight_copies:
                copies[2].wait_recv()

    def pass_all():
        for c in range(PIECES):
            pass_on(c)
        incoming[1, 0] = outgoing[1, spot]

    far = list(range(1, bands))
    pl.when(early)(pass_all)
    rise((0, 0, 0), (0, 0, 0))

    @pl.when(early)
    def _():
        for r in outside:
            slot_copy(0, r, 0).start()

    rise((1, 0, 1), (0, 1, 1))
    for k in far[1:]:
        rise(None, (0, k, k))
    pl.when(late)(pass_all)
    down_weights()
    fall((0, 0, 0), (0, 0, 0))
    for k in far:
        fall(None, (0, k, k))
    for copy in count_copies:
        copy.wait()
    half_total = counts[0]
    for r in range(1, kept_steps):
        half_total = half_total + counts[r]
    half_counts[0] = half_total
    pair_copy = remote(half_counts.at[0], half_counts.at[1], pair_send, pair_recv, other)
    pair_copy.start()
    rise((1, 1, bands), (1, 0, 0))
    for k in far[1:]:
        rise((1, k, bands - 1 + k), (1, k - 1, bands - 2 + k))
    rise(None, (1, bands - 1, 2 * bands - 2))
    for k in far:
        fall((1, k, bands - 1 + k), (1, k, bands - 1 + k))
    fall((1, 0, 1), (1, 0, 0))
    for k in far:
        rise((0, k, 0), None)
        fall((0, k, 0), None)
    for u in range(2):
        returned[u, spot] = answers[u, 0]

    half_copies = [
        remote(halves.at[0, c], halves.at[1, c], half_send.at[c], half_recv.at[c], other)
        for c in range(CHUNKS)
    ]
    for c in range(CHUNKS):
        with scope(f"arrived1{c}"):
            arrived(1, c)
        halves[0, c] = mixture(1, c).astype(jnp.bfloat16)
        half_copies[c].start()

    with scope("counts"):
        pair_copy.wait()
    class_count[...] = half_counts[0] + half_counts[1]
    group_copies = [
        remote(class_count, group_counts.at[t], group_send.at[t], group_recv.at[t], address(place, peers[t]))
        for t in range(1, groups)
    ]
    for copy in group_copies:
        copy.start()

    for c in range(CHUNKS):
        with scope(f"arrived0{c}"):
            arrived(0, c)
        total[:, c * chunk : (c + 1) * chunk] = frames[:, c * chunk : (c + 1) * chunk].astype(
            jnp.float32
        ) + mixture(0, c)
    with scope("groupwait"):
        for copy in group_copies:
            copy.wait()
    everything = class_count[...]
    for t in range(1, groups):
        everything = everything + group_counts[t]
    load[...] = everything

    fact_done = [copy for copies in weight_copies for copy in copies]
    for copy in fact_done:
        copy.wait_send()
    for r in inside:
        slot_copy(0, r, 0).wait_send()

    @pl.when(early)
    def _():
        for r in outside:
            slot_copy(0, r, 0).wait_send()

    for copy in shared_copies:
        copy.wait_send()

    for r in range(1, kept_steps):
        for c in range(PIECES):
            slot_copy(1, r, c).wait_send()
        for u in range(2):
            for c in range(CHUNKS):
                back_copy(u, r, c).wait_send()
    for c in range(CHUNKS):
        with scope(f"halfwait{c}"):
            half_copies[c].wait()
        mixed[:, c * chunk : (c + 1) * chunk] = (
            total[:, c * chunk : (c + 1) * chunk] + halves[1, c].astype(jnp.float32)
        ).astype(jnp.bfloat16)


def finish_kernel(mixed, load, mixed_out, load_out):
    mixed_out[...] = mixed[...]
    load_out[...] = load[0:1, 0 : load_out.shape[1]]


def per_device(
    frames,
    norm_gain,
    norm_bias,
    routes,
    gate_codes,
    limits,
    up_weight,
    up_bias,
    down_weight,
    down_bias,
):
    owners = lax.axis_size("dp")
    holders = lax.axis_size("expert")
    expert_total = down_bias.shape[0]
    groups = owners * holders // expert_total
    frame_count, width = frames.shape
    capacity = 4 * frame_count // expert_total
    hidden_units = up_weight.shape[2]
    vmem = pl.BlockSpec(memory_space=pltpu.VMEM)
    anywhere = pl.BlockSpec(memory_space=pl.ANY)
    kept_steps = expert_total // 2
    slots = kept_steps * capacity
    blocks = (2, kept_steps, capacity, width)
    dma = pltpu.SemaphoreType.DMA
    mixed, load = pl.pallas_call(
        functools.partial(moe_kernel, owners, holders, groups, capacity),
        out_shape=(
            pltpu.VMEM((frame_count, width), jnp.bfloat16),
            pltpu.VMEM((8, 128), jnp.int32),
        ),
        in_specs=[
            anywhere,
            anywhere,
            anywhere,
            anywhere,
            anywhere,
            anywhere,
            anywhere,
            anywhere,
            anywhere,
            anywhere,
        ],
        out_specs=(vmem, vmem),
        scratch_shapes=[
            pltpu.SMEM((expert_total,), jnp.int32),
            pltpu.VMEM((frame_count, width), jnp.bfloat16),
            pltpu.VMEM((1, width), jnp.float32),
            pltpu.VMEM((1, width), jnp.float32),
            pltpu.VMEM((2, frame_count), jnp.int32),
            pltpu.VMEM((2, frame_count), jnp.int32),
            pltpu.VMEM((expert_total, width), jnp.float32),
            pltpu.VMEM((groups, width, hidden_units), jnp.bfloat16),
            pltpu.VMEM((groups, hidden_units, width), jnp.bfloat16),
            pltpu.VMEM((groups, 1, hidden_units), jnp.float32),
            pltpu.VMEM((2, 8, frame_count), jnp.int32),
            pltpu.VMEM((2, PIECES, frame_count, width // PIECES), jnp.bfloat16),
            pltpu.VMEM(blocks, jnp.bfloat16),
            pltpu.VMEM(blocks, jnp.bfloat16),
            pltpu.VMEM((owners - 1, slots // (owners // 2), groups * hidden_units), jnp.bfloat16),
            pltpu.VMEM(blocks, jnp.bfloat16),
            pltpu.VMEM(blocks, jnp.bfloat16),
            pltpu.VMEM((2, CHUNKS, frame_count, width // CHUNKS), jnp.bfloat16),
            pltpu.VMEM((kept_steps, 8, 128), jnp.int32),
            pltpu.VMEM((2, 8, 128), jnp.int32),
            pltpu.VMEM((8, 128), jnp.int32),
            pltpu.VMEM((groups, 8, 128), jnp.int32),
            pltpu.VMEM((2, frame_count, slots), jnp.bfloat16),
            pltpu.VMEM((2, frame_count, slots), jnp.bfloat16),
            pltpu.VMEM((frame_count, width), jnp.float32),
            dma((8,)),
            dma((2,)),
            dma((groups, 3)),
            dma((groups, 3)),
            dma(()),
            dma(()),
            dma((PIECES,)),
            dma((PIECES,)),
            dma((2, kept_steps, PIECES)),
            dma((2, kept_steps, PIECES)),
            dma((2, kept_steps, CHUNKS)),
            dma((2, kept_steps, CHUNKS)),
            dma((CHUNKS,)),
            dma((CHUNKS,)),
            dma((kept_steps,)),
            dma((kept_steps,)),
            dma(()),
            dma(()),
            dma((groups,)),
            dma((groups,)),
        ],
        compiler_params=pltpu.CompilerParams(
            collective_id=0, has_side_effects=True, vmem_limit_bytes=56 * 1024 * 1024
        ),
        name="moe",
    )(
        limits,
        frames,
        norm_gain.reshape(1, width),
        norm_bias.reshape(1, width),
        routes.T,
        gate_codes.T,
        up_weight,
        up_bias,
        down_weight,
        down_bias,
    )
    mixed, load = pl.pallas_call(
        finish_kernel,
        out_shape=(
            jax.ShapeDtypeStruct((frame_count, width), jnp.bfloat16),
            jax.ShapeDtypeStruct((1, expert_total), jnp.int32),
        ),
        in_specs=[vmem, vmem],
        out_specs=(vmem, vmem),
        compiler_params=pltpu.CompilerParams(vmem_limit_bytes=2 * 1024 * 1024),
        name="finish",
    )(mixed, load)
    return (mixed, load.reshape(expert_total))


def solution(mesh):
    in_specs = (
        P(("dp", "expert"), None),
        P(),
        P(),
        P(("dp", "expert"), None),
        P(("dp", "expert"), None),
        P(),
        P(("dp", "expert"), None, None),
        P(("dp", "expert"), None),
        P(("dp", "expert"), None, None),
        P(),
    )
    out_specs = (P(("dp", "expert"), None), P())
    return jax.shard_map(
        per_device, mesh=mesh, in_specs=in_specs, out_specs=out_specs, check_vma=False
    )
```

```python
import functools
import jax
import jax.numpy as jnp
from jax import lax
from jax.experimental import pallas as pl
from jax.experimental.pallas import tpu as pltpu
from jax.sharding import PartitionSpec as P

epsilon = 1e-05
TILE = 512
PIECES = 4
CHUNKS = 4
WIDE = 2


def paired(value, step, size):
    bit = 1
    out = value
    while bit < size:
        if step & bit:
            out = out + bit - 2 * bit * lax.rem(value // bit, 2)
        bit *= 2
    return out


def moe_kernel(
    owners,
    holders,
    groups,
    capacity,
    limits_in,
    frames_in,
    gain_in,
    bias_in,
    routes_in,
    codes_in,
    up_weight,
    up_bias,
    down_weight,
    down_bias_in,
    mixed,
    load,
    limits,
    frames,
    gain,
    bias,
    routes,
    codes,
    down_bias,
    up_all,
    down_all,
    bias_all,
    facts,
    shared,
    outgoing,
    incoming,
    hidden,
    answers,
    returned,
    halves,
    counts,
    half_counts,
    class_count,
    group_counts,
    mix_high,
    mix_low,
    total,
    load_sem,
    own_sem,
    weight_send,
    weight_recv,
    fact_send,
    fact_recv,
    shared_send,
    shared_recv,
    slot_send,
    slot_recv,
    back_send,
    back_recv,
    half_send,
    half_recv,
    count_send,
    count_recv,
    pair_send,
    pair_recv,
    group_send,
    group_recv,
):
    row = lax.axis_index("dp")
    column = lax.axis_index("expert")
    near = holders // groups
    flat = row * holders + column
    place = flat // groups
    member = lax.rem(flat, groups)
    band = place // near
    spot = lax.rem(place, near)
    early = lax.rem(member, 2) == 0
    late = lax.rem(member, 2) == 1
    frame_count, width = frames.shape
    hidden_units = up_weight.shape[2]
    bands = owners // 2
    kept_steps = bands * near
    slots = kept_steps * capacity
    block = near * capacity
    part = width // PIECES
    chunk = width // CHUNKS
    scope = jax.named_scope

    def address(expert, group):
        number = expert * groups + group
        return (number // holders, lax.rem(number, holders))

    def remote(source, target, send, recv, to):
        return pltpu.make_async_remote_copy(
            src_ref=source,
            dst_ref=target,
            send_sem=send,
            recv_sem=recv,
            device_id=to,
            device_id_type=pl.DeviceIdType.MESH,
        )

    spots = [paired(spot, j, near) for j in range(near)]
    to_band = [paired(band, k, owners) for k in range(owners)]
    ahead = [to_band[k] * near + spots[j] for k in range(owners) for j in range(near)]
    peers = [lax.rem(member + t, groups) for t in range(groups)]

    barrier = pltpu.get_barrier_semaphore()
    other = address(to_band[bands] * near + spot, member)
    pl.semaphore_signal(barrier, inc=1, device_id=other, device_id_type=pl.DeviceIdType.MESH)
    for r in range(1, kept_steps):
        pl.semaphore_signal(
            barrier, inc=1, device_id=address(ahead[r], member), device_id_type=pl.DeviceIdType.MESH
        )
    for t in range(1, groups):
        pl.semaphore_signal(
            barrier, inc=1, device_id=address(place, peers[t]), device_id_type=pl.DeviceIdType.MESH
        )
    loads = [
        pltpu.make_async_copy(source, target, load_sem.at[i])
        for i, (source, target) in enumerate(
            (
                (frames_in, frames),
                (gain_in, gain),
                (bias_in, bias),
                (routes_in, routes),
                (codes_in, codes),
                (limits_in, limits),
                (up_bias, bias_all.at[0]),
                (down_bias_in, down_bias),
            )
        )
    ]
    for copy in loads:
        copy.start()
    own = [
        pltpu.make_async_copy(up_weight.at[0], up_all.at[0], own_sem.at[0]),
        pltpu.make_async_copy(down_weight.at[0], down_all.at[0], own_sem.at[1]),
    ]
    for copy in loads[:3]:
        copy.wait()

    values = frames[...].astype(jnp.float32)
    center = jnp.mean(values, axis=-1, keepdims=True)
    shifted = values - center
    spread = jnp.mean(shifted * shifted, axis=-1, keepdims=True)
    normed = (shifted * lax.rsqrt(spread + epsilon) * gain[...] + bias[...]).astype(jnp.bfloat16)
    for c in range(PIECES):
        shared[0, c] = normed[:, c * part : (c + 1) * part]
    for copy in loads[3:]:
        copy.wait()
    facts[0, 0:2, :] = routes[...]
    facts[0, 2:4, :] = codes[...]
    facts[0, 4:8, :] = jnp.zeros((4, frame_count), jnp.int32)
    for copy in own:
        copy.start()

    square = (frame_count, frame_count)
    across = lax.broadcasted_iota(jnp.int32, square, 1)
    along = lax.broadcasted_iota(jnp.int32, square, 0)
    earlier = jnp.where(across < along, 1.0, 0.0).astype(jnp.bfloat16)
    diagonal = across == along
    lane = lax.broadcasted_iota(jnp.int32, (1, slots), 1)
    line = lane // capacity
    slot_of = lax.rem(lane, capacity).astype(jnp.float32)

    def expert_at(q):
        return to_band[q // near] * near + q % near

    def experts(numbers):
        out = jnp.zeros(numbers.shape, jnp.int32)
        for q in range(kept_steps):
            out = jnp.where(numbers == q, expert_at(q), out)
        return out

    expert_of = experts(line)
    bound = jnp.zeros((1, slots), jnp.int32)
    for q in range(kept_steps):
        bound = jnp.where(line == q, limits[expert_at(q)], bound)
    bound = bound.astype(jnp.float32)
    tall = lax.broadcasted_iota(jnp.int32, (slots, 128), 0) // capacity
    to_lane = experts(tall) == lax.broadcasted_iota(jnp.int32, (slots, 128), 1)
    to_lane = jnp.where(to_lane, 1.0, 0.0).astype(jnp.bfloat16)

    def places(u):
        def upright(i):
            lying = facts[u, i : i + 1, :].astype(jnp.float32)
            return jnp.sum(jnp.where(diagonal, lying, 0.0), axis=1, keepdims=True)

        first, second = upright(0).astype(jnp.int32), upright(1).astype(jnp.int32)
        first_code, second_code = upright(2), upright(3)
        code_sum = first_code + second_code
        first_share, second_share = first_code / code_sum, second_code / code_sum
        hit_first, hit_second = first == expert_of, second == expert_of
        hits = jnp.where(hit_first | hit_second, 1.0, 0.0)
        rank = jnp.dot(earlier, hits.astype(jnp.bfloat16), preferred_element_type=jnp.float32)
        fits = (rank == slot_of) & (rank < bound)
        chosen = jnp.where(fits, hits, 0.0)
        picked = chosen.astype(jnp.bfloat16)
        mix = chosen * jnp.where(hit_first, first_share, second_share)
        high = mix.astype(jnp.bfloat16)
        mix_high[u] = high
        mix_low[u] = (mix - high.astype(jnp.float32)).astype(jnp.bfloat16)
        tally = jnp.dot(picked, to_lane, preferred_element_type=jnp.float32)
        return picked, jnp.sum(tally, axis=0, keepdims=True)

    def fill(u, begin, size, picked, source):
        rows = lax.dot_general(
            picked, source, (((0,), (0,)), ((), ())), preferred_element_type=jnp.float32
        )
        outgoing[u, :, :, begin : begin + size] = rows.astype(jnp.bfloat16).reshape(
            kept_steps, capacity, size
        )

    def slot_copy(u, r, c):
        k, j = r // near, r % near
        columns = pl.ds(c * part, part) if u else pl.ds(0, width)
        return remote(
            outgoing.at[u, k * near + spots[j], :, columns],
            incoming.at[u, r, :, columns],
            slot_send.at[u, r, c],
            slot_recv.at[u, r, c],
            address(ahead[r], member),
        )

    inside = list(range(1, near))
    outside = list(range(near, kept_steps))

    with scope("barrier"):
        pl.semaphore_wait(barrier, kept_steps + groups - 1)
    fact_copy = remote(facts.at[0], facts.at[1], fact_send, fact_recv, other)
    fact_copy.start()
    shared_copies = [
        remote(shared.at[0, c], shared.at[1, c], shared_send.at[c], shared_recv.at[c], other)
        for c in range(PIECES)
    ]

    @pl.when(early)
    def _():
        for copy in shared_copies:
            copy.start()

    weight_copies = []
    for t in range(1, groups):
        to = address(place, peers[t])
        weight_copies.append([
            remote(bias_all.at[0], bias_all.at[t], weight_send.at[t, 0], weight_recv.at[t, 0], to),
            remote(up_weight.at[0], up_all.at[t], weight_send.at[t, 1], weight_recv.at[t, 1], to),
            remote(down_weight.at[0], down_all.at[t], weight_send.at[t, 2], weight_recv.at[t, 2], to),
        ])
    for i in range(3):
        for copies in weight_copies:
            copies[i].start()

    with scope("fill0"):
        own_picks, own_tally = places(0)
        fill(0, 0, width, own_picks, normed)
    for r in inside:
        slot_copy(0, r, 0).start()
    incoming[0, 0] = outgoing[0, spot]

    @pl.when(late)
    def _():
        for r in outside:
            slot_copy(0, r, 0).start()
        with scope("slotsend"):
            for r in outside:
                slot_copy(0, r, 0).wait_send()
        for copy in shared_copies:
            copy.start()

    with scope("factwait"):
        fact_copy.wait()
    with scope("places1"):
        other_picks, other_tally = places(1)
    counts[0] = jnp.broadcast_to((own_tally + other_tally).astype(jnp.int32), (8, 128))
    count_copies = [
        remote(counts.at[0], counts.at[r], count_send.at[r], count_recv.at[r], address(ahead[r], member))
        for r in range(1, kept_steps)
    ]
    for copy in count_copies:
        copy.start()

    def pass_on(c):
        with scope(f"sharedwait{c}"):
            shared_copies[c].wait_recv()
        fill(1, c * part, part, other_picks, shared[1, c])
        for r in outside + inside:
            slot_copy(1, r, c).start()

    out_bias = down_bias[pl.ds(place, 1), :]
    tile = min(TILE, hidden_units)

    def up(u, k, at, first):
        for t in range(groups):
            if first:
                with scope(f"upweight{t}"):
                    if t:
                        weight_copies[t - 1][0].wait_recv()
                        weight_copies[t - 1][1].wait_recv()
                    else:
                        own[0].wait()
            for i in range(hidden_units // tile):
                pre = jnp.dot(
                    incoming[u, pl.ds(k * near, near)].reshape(block, width),
                    up_all[t, :, i * tile : (i + 1) * tile],
                    preferred_element_type=jnp.float32,
                )
                pre = pre + bias_all[t, :, i * tile : (i + 1) * tile]
                begin = t * hidden_units + i * tile
                hidden[at, :, begin : begin + tile] = (
                    0.5 * pre * (1.0 + lax.erf(pre * 0.7071067811865476))
                ).astype(jnp.bfloat16)

    def back_copy(u, r, c):
        k = r // near
        columns = pl.ds(c * chunk, chunk)
        return remote(
            answers.at[u, r, :, columns],
            returned.at[u, k * near + spot, :, columns],
            back_send.at[u, r, c],
            back_recv.at[u, r, c],
            address(ahead[r], member),
        )

    def down(u, k, at, c):
        begin, end = c * width // WIDE, (c + 1) * width // WIDE
        sums = out_bias[:, begin:end]
        for t in range(groups):
            sums = sums + jnp.dot(
                hidden[at, :, t * hidden_units : (t + 1) * hidden_units],
                down_all[t, :, begin:end],
                preferred_element_type=jnp.float32,
            )
        answers[u, pl.ds(k * near, near), :, begin:end] = sums.astype(jnp.bfloat16).reshape(
            near, capacity, end - begin
        )

    def arrived(u, c):
        for r in range(1, kept_steps):
            k, j = r // near, r % near
            columns = pl.ds(c * chunk, chunk)
            remote(
                answers.at[u, r, :, columns],
                returned.at[u, k * near + spots[j], :, columns],
                back_send.at[u, r, c],
                back_recv.at[u, r, c],
                address(ahead[r], member),
            ).wait_recv()

    def mixture(u, c):
        picked = returned[u, :, :, c * chunk : (c + 1) * chunk].reshape(slots, chunk)
        return jnp.dot(mix_high[u], picked, preferred_element_type=jnp.float32) + jnp.dot(
            mix_low[u], picked, preferred_element_type=jnp.float32
        )

    def rows_wait(u, k):
        for r in range(max(1, k * near), (k + 1) * near):
            for c in range(PIECES if u else 1):
                slot_copy(u, r, c).wait_recv()

    def back_start(u, k, c):
        for r in range(max(1, k * near), (k + 1) * near):
            back_copy(u, r, c).start()

    def by_member(one, two, act):
        if one == two:
            act(one)
            return
        for item, mine in ((one, early), (two, late)):
            if item is not None:
                pl.when(mine)(functools.partial(act, item))

    def both(one, two):
        return [a if a == b else jnp.where(early, a, b) for a, b in zip(one, two)]

    def rise(one, two):
        def act(item):
            with scope(f"up_{item[0]}{item[1]}"):
                up(*item, False)

        def rows(item):
            with scope(f"rows_{item[0]}{item[1]}"):
                rows_wait(item[0], item[1])

        by_member(one, two, rows)
        if one is None or two is None:
            by_member(one, two, act)
        else:
            with scope("up"):
                up(*both(one, two), one == two)

    def fall(one, two):
        for w in range(WIDE):
            if one is None or two is None:
                by_member(one, two, lambda item: down(*item, w))
            else:
                with scope(f"down{w}"):
                    down(*both(one, two), w)
            for c in range(w * CHUNKS // WIDE, (w + 1) * CHUNKS // WIDE):
                by_member(one, two, lambda item: back_start(item[0], item[1], c))

    def down_weights():
        with scope("downweight"):
            own[1].wait()
            for copies in weight_copies:
                copies[2].wait_recv()

    def pass_all():
        for c in range(PIECES):
            pass_on(c)
        incoming[1, 0] = outgoing[1, spot]

    far = list(range(1, bands))
    pl.when(early)(pass_all)
    rise((0, 0, 0), (0, 0, 0))

    @pl.when(early)
    def _():
        for r in outside:
            slot_copy(0, r, 0).start()

    rise((1, 0, 1), (0, 1, 1))
    for k in far[1:]:
        rise(None, (0, k, k))
    pl.when(late)(pass_all)
    down_weights()
    fall((0, 0, 0), (0, 0, 0))
    for k in far:
        fall(None, (0, k, k))
    for copy in count_copies:
        copy.wait()
    half_total = counts[0]
    for r in range(1, kept_steps):
        half_total = half_total + counts[r]
    half_counts[0] = half_total
    pair_copy = remote(half_counts.at[0], half_counts.at[1], pair_send, pair_recv, other)
    pair_copy.start()
    rise((1, 1, bands), (1, 0, 0))
    for k in far[1:]:
        rise((1, k, bands - 1 + k), (1, k - 1, bands - 2 + k))
    rise(None, (1, bands - 1, 2 * bands - 2))
    for k in far:
        fall((1, k, bands - 1 + k), (1, k, bands - 1 + k))
    fall((1, 0, 1), (1, 0, 0))
    for k in far:
        rise((0, k, 0), None)
        fall((0, k, 0), None)
    for u in range(2):
        returned[u, spot] = answers[u, 0]

    half_copies = [
        remote(halves.at[0, c], halves.at[1, c], half_send.at[c], half_recv.at[c], other)
        for c in range(CHUNKS)
    ]
    for c in range(CHUNKS):
        with scope(f"arrived1{c}"):
            arrived(1, c)
        halves[0, c] = mixture(1, c).astype(jnp.bfloat16)
        half_copies[c].start()

    with scope("counts"):
        pair_copy.wait()
    class_count[...] = half_counts[0] + half_counts[1]
    group_copies = [
        remote(class_count, group_counts.at[t], group_send.at[t], group_recv.at[t], address(place, peers[t]))
        for t in range(1, groups)
    ]
    for copy in group_copies:
        copy.start()

    for c in range(CHUNKS):
        with scope(f"arrived0{c}"):
            arrived(0, c)
        total[:, c * chunk : (c + 1) * chunk] = frames[:, c * chunk : (c + 1) * chunk].astype(
            jnp.float32
        ) + mixture(0, c)
    with scope("groupwait"):
        for copy in group_copies:
            copy.wait()
    everything = class_count[...]
    for t in range(1, groups):
        everything = everything + group_counts[t]
    load[...] = everything

    fact_done = [copy for copies in weight_copies for copy in copies]
    for copy in fact_done:
        copy.wait_send()
    for r in inside:
        slot_copy(0, r, 0).wait_send()

    @pl.when(early)
    def _():
        for r in outside:
            slot_copy(0, r, 0).wait_send()

    for copy in shared_copies:
        copy.wait_send()

    for r in range(1, kept_steps):
        for c in range(PIECES):
            slot_copy(1, r, c).wait_send()
        for u in range(2):
            for c in range(CHUNKS):
                back_copy(u, r, c).wait_send()
    for c in range(CHUNKS):
        with scope(f"halfwait{c}"):
            half_copies[c].wait()
        mixed[:, c * chunk : (c + 1) * chunk] = (
            total[:, c * chunk : (c + 1) * chunk] + halves[1, c].astype(jnp.float32)
        ).astype(jnp.bfloat16)


def finish_kernel(mixed, load, mixed_out, load_out):
    mixed_out[...] = mixed[...]
    load_out[...] = load[0:1, 0 : load_out.shape[1]]


def per_device(
    frames,
    norm_gain,
    norm_bias,
    routes,
    gate_codes,
    limits,
    up_weight,
    up_bias,
    down_weight,
    down_bias,
):
    owners = lax.axis_size("dp")
    holders = lax.axis_size("expert")
    expert_total = down_bias.shape[0]
    groups = owners * holders // expert_total
    frame_count, width = frames.shape
    capacity = 4 * frame_count // expert_total
    hidden_units = up_weight.shape[2]
    vmem = pl.BlockSpec(memory_space=pltpu.VMEM)
    anywhere = pl.BlockSpec(memory_space=pl.ANY)
    kept_steps = expert_total // 2
    slots = kept_steps * capacity
    blocks = (2, kept_steps, capacity, width)
    dma = pltpu.SemaphoreType.DMA
    mixed, load = pl.pallas_call(
        functools.partial(moe_kernel, owners, holders, groups, capacity),
        out_shape=(
            pltpu.VMEM((frame_count, width), jnp.bfloat16),
            pltpu.VMEM((8, 128), jnp.int32),
        ),
        in_specs=[
            anywhere,
            anywhere,
            anywhere,
            anywhere,
            anywhere,
            anywhere,
            anywhere,
            anywhere,
            anywhere,
            anywhere,
        ],
        out_specs=(vmem, vmem),
        scratch_shapes=[
            pltpu.SMEM((expert_total,), jnp.int32),
            pltpu.VMEM((frame_count, width), jnp.bfloat16),
            pltpu.VMEM((1, width), jnp.float32),
            pltpu.VMEM((1, width), jnp.float32),
            pltpu.VMEM((2, frame_count), jnp.int32),
            pltpu.VMEM((2, frame_count), jnp.int32),
            pltpu.VMEM((expert_total, width), jnp.float32),
            pltpu.VMEM((groups, width, hidden_units), jnp.bfloat16),
            pltpu.VMEM((groups, hidden_units, width), jnp.bfloat16),
            pltpu.VMEM((groups, 1, hidden_units), jnp.float32),
            pltpu.VMEM((2, 8, frame_count), jnp.int32),
            pltpu.VMEM((2, PIECES, frame_count, width // PIECES), jnp.bfloat16),
            pltpu.VMEM(blocks, jnp.bfloat16),
            pltpu.VMEM(blocks, jnp.bfloat16),
            pltpu.VMEM((owners - 1, slots // (owners // 2), groups * hidden_units), jnp.bfloat16),
            pltpu.VMEM(blocks, jnp.bfloat16),
            pltpu.VMEM(blocks, jnp.bfloat16),
            pltpu.VMEM((2, CHUNKS, frame_count, width // CHUNKS), jnp.bfloat16),
            pltpu.VMEM((kept_steps, 8, 128), jnp.int32),
            pltpu.VMEM((2, 8, 128), jnp.int32),
            pltpu.VMEM((8, 128), jnp.int32),
            pltpu.VMEM((groups, 8, 128), jnp.int32),
            pltpu.VMEM((2, frame_count, slots), jnp.bfloat16),
            pltpu.VMEM((2, frame_count, slots), jnp.bfloat16),
            pltpu.VMEM((frame_count, width), jnp.float32),
            dma((8,)),
            dma((2,)),
            dma((groups, 3)),
            dma((groups, 3)),
            dma(()),
            dma(()),
            dma((PIECES,)),
            dma((PIECES,)),
            dma((2, kept_steps, PIECES)),
            dma((2, kept_steps, PIECES)),
            dma((2, kept_steps, CHUNKS)),
            dma((2, kept_steps, CHUNKS)),
            dma((CHUNKS,)),
            dma((CHUNKS,)),
            dma((kept_steps,)),
            dma((kept_steps,)),
            dma(()),
            dma(()),
            dma((groups,)),
            dma((groups,)),
        ],
        compiler_params=pltpu.CompilerParams(
            collective_id=0, has_side_effects=True, vmem_limit_bytes=56 * 1024 * 1024
        ),
        name="moe",
    )(
        limits,
        frames,
        norm_gain.reshape(1, width),
        norm_bias.reshape(1, width),
        routes.T,
        gate_codes.T,
        up_weight,
        up_bias,
        down_weight,
        down_bias,
    )
    mixed, load = pl.pallas_call(
        finish_kernel,
        out_shape=(
            jax.ShapeDtypeStruct((frame_count, width), jnp.bfloat16),
            jax.ShapeDtypeStruct((1, expert_total), jnp.int32),
        ),
        in_specs=[vmem, vmem],
        out_specs=(vmem, vmem),
        compiler_params=pltpu.CompilerParams(vmem_limit_bytes=2 * 1024 * 1024),
        name="finish",
    )(mixed, load)
    return (mixed, load.reshape(expert_total))


def solution(mesh):
    in_specs = (
        P(("dp", "expert"), None),
        P(),
        P(),
        P(("dp", "expert"), None),
        P(("dp", "expert"), None),
        P(),
        P(("dp", "expert"), None, None),
        P(("dp", "expert"), None),
        P(("dp", "expert"), None, None),
        P(),
    )
    out_specs = (P(("dp", "expert"), None), P())
    return jax.shard_map(
        per_device, mesh=mesh, in_specs=in_specs, out_specs=out_specs, check_vma=False
    )
```
